32 devices in a mesh: seq: 16 (over z, x, core), head: 2 (over y).
Axes of the slice: x: 2, y: 2, z: 4, core: 2. Of those that a mesh axis runs over, the one named last changes fastest.
Arguments:
- queries: bfloat16 [8192, 4096], P('seq', 'head'), may hold values from -1.8 to 1.8
- keys: bfloat16 [8192, 4096], P('seq', 'head'), may hold values from -1.8 to 1.8
- values: bfloat16 [8192, 4096], P('seq', 'head'), may hold values from -6 to 6
- gain: float32 [4096], P('head'), may hold values from 0.25 to 1.75
- cotangent: bfloat16 [8192, 4096], P('seq', 'head'), may hold values from -6 to 6
Outputs:
- normed_out: bfloat16 [8192, 4096], P('seq', 'head')
- grad_queries: bfloat16 [8192, 4096], P('seq', 'head')
- grad_keys: bfloat16 [8192, 4096], P('seq', 'head')
- grad_values: bfloat16 [8192, 4096], P('seq', 'head')
The draws below stay inside these ranges and needn't reach their ends.
All inputs are finite; a program needn't handle non-finite values.
Results may differ from the reference program's by a relative error of at most 0.0064.
Values sent between devices are 32-bit elements; how exact they have to be, the bound alone decides.
No kernel may reach another device: no remote copies, remote signals or barrier semaphores. Data moves between devices by JAX's collectives and lax.ppermute only.
A program may use at most 128 MiB of HBM per device.

```python
import math
import jax
import jax.numpy as jnp
from jax import lax

H = 32
DH = 128
TOK_DEV = 512
TOKENS = 8192
D = 4096


SPREADS = (0.3, 0.3, 1.0)


def drawn_field(key, number):
    subkey = jax.random.fold_in(key, 101 + number)
    spread = SPREADS[number]
    if number == 2:
        scale_key = jax.random.fold_in(key, 211)
        head_scales = jnp.exp(jax.random.uniform(scale_key, (H,), jnp.float32, math.log(0.4), math.log(4.0)))
        column_scale = jnp.repeat(head_scales, DH)[None, :]
    else:
        column_scale = jnp.ones((1, D), jnp.float32)
    sample = spread * jax.random.normal(subkey, (TOKENS, D), jnp.float32)
    return jnp.clip(sample * column_scale, -6.0 * spread, 6.0 * spread).astype(jnp.bfloat16)


def normalized_output(key):
    blocks = TOKENS // TOK_DEV

    def by_head(array):
        return array.astype(jnp.float32).reshape(blocks, TOK_DEV, H, DH)
    query_blocks = by_head(drawn_field(key, 0))
    key_blocks = by_head(drawn_field(key, 1))
    value_blocks = by_head(drawn_field(key, 2))
    row_ids = lax.broadcasted_iota(jnp.int32, (TOK_DEV, TOK_DEV), 0)
    col_ids = lax.broadcasted_iota(jnp.int32, (TOK_DEV, TOK_DEV), 1)
    causal = (row_ids >= col_ids)[None]

    def forward(running, inputs):
        query_block, key_block, value_block = inputs
        scores = jnp.where(causal, jnp.einsum('thi,shi->hts', query_block, key_block), 0.0)
        attend = jnp.einsum('hts,shj->thj', scores, value_block) + jnp.einsum('thi,hij->thj', query_block, running)
        return (running + jnp.einsum('thi,thj->hij', key_block, value_block), attend)
    empty = jnp.zeros((H, DH, DH), jnp.float32)
    _, attend = lax.scan(forward, empty, (query_blocks, key_blocks, value_blocks))
    attend = attend.reshape(TOKENS, D)
    mean_square = jnp.mean(attend * attend, axis=1, keepdims=True)
    return attend / jnp.sqrt(mean_square + 1e-06)


def draw_queries(key, part):
    return drawn_field(key, 0)


def draw_keys(key, part):
    return drawn_field(key, 1)


def draw_values(key, part):
    return drawn_field(key, 2)


def draw_cotangent(key, part):
    normed = normalized_output(key)
    noise_key = jax.random.fold_in(key, 307)
    mixed = 0.5 * normed + 0.8 * jax.random.normal(noise_key, (TOKENS, D), jnp.float32)
    return jnp.clip(mixed, -6.0, 6.0).astype(jnp.bfloat16)


def setup_inputs(seed: int = 0) -> dict:
    seeds = jax.random.split(jax.random.key(seed), 6)
    queries = draw_queries(jax.random.fold_in(seeds[5], 71), 0)
    keys = draw_keys(jax.random.fold_in(seeds[5], 71), 0)
    values = draw_values(jax.random.fold_in(seeds[5], 71), 0)
    gain = jnp.clip(1.0 + 0.15 * jax.random.normal(seeds[3], (D,), jnp.float32), 0.25, 1.75)
    cotangent = draw_cotangent(jax.random.fold_in(seeds[5], 71), 0)
    return {"queries": queries, "keys": keys, "values": values, "gain": gain, "cotangent": cotangent}


EPSILON = 1e-06

def rounded(array):
    return lax.optimization_barrier(array.astype(jnp.bfloat16)).astype(jnp.float32)

def reference(queries, keys, values, gain, cotangent):
    blocks = queries.shape[0] // TOK_DEV
    head_count = gain.shape[0] // DH
    model_width = head_count * DH

    def by_head(array):
        return array.reshape(blocks, TOK_DEV, head_count, DH).astype(jnp.float32)
    query_blocks, key_blocks, value_blocks = (by_head(queries), by_head(keys), by_head(values))
    row_ids = lax.broadcasted_iota(jnp.int32, (TOK_DEV, TOK_DEV), 0)
    col_ids = lax.broadcasted_iota(jnp.int32, (TOK_DEV, TOK_DEV), 1)
    causal = row_ids >= col_ids

    def scores_of(query_block, key_block):
        scores = jnp.einsum('thi,shi->hts', query_block, key_block)
        return rounded(jnp.where(causal[None], scores, 0.0))

    def forward(running, inputs):
        query_block, key_block, value_block = inputs
        scores = scores_of(query_block, key_block)
        attend = jnp.einsum('hts,shj->thj', scores, value_block) + jnp.einsum('thi,hij->thj', query_block, rounded(running))
        return (running + jnp.einsum('thi,thj->hij', key_block, value_block), (attend, running))
    empty = jnp.zeros((head_count, DH, DH), jnp.float32)
    _, (attend, prefixes) = lax.scan(forward, empty, (query_blocks, key_blocks, value_blocks))
    attend = attend.reshape(blocks * TOK_DEV, model_width)
    mean_square = lax.optimization_barrier(jnp.sum(attend * attend, axis=1, keepdims=True)) / model_width
    inverse = 1.0 / jnp.sqrt(mean_square + EPSILON)
    normed = attend * inverse
    normed_out = (normed * gain).astype(jnp.bfloat16)
    scaled_grad = cotangent.astype(jnp.float32) * gain
    slope = lax.optimization_barrier(jnp.sum(scaled_grad * normed, axis=1, keepdims=True)) / model_width
    grad_attn = (inverse * (scaled_grad - normed * slope)).astype(jnp.bfloat16)
    grad_blocks = by_head(grad_attn)

    def backward(suffix, inputs):
        query_block, key_block, value_block, grad_block, prefix_state = inputs
        scores = scores_of(query_block, key_block)
        grad_scores = rounded(jnp.where(causal[None], jnp.einsum('thj,shj->hts', grad_block, value_block), 0.0))
        suffix_low = rounded(suffix)
        grad_q = jnp.einsum('hts,shi->thi', grad_scores, key_block) + jnp.einsum('thj,hij->thi', grad_block, rounded(prefix_state))
        grad_k = jnp.einsum('hts,thi->shi', grad_scores, query_block) + jnp.einsum('shj,hij->shi', value_block, suffix_low)
        grad_v = jnp.einsum('hts,thj->shj', scores, grad_block) + jnp.einsum('shi,hij->shj', key_block, suffix_low)
        return (suffix + jnp.einsum('thi,thj->hij', query_block, grad_block), (grad_q, grad_k, grad_v))
    _, (grad_q, grad_k, grad_v) = lax.scan(backward, empty, (query_blocks, key_blocks, value_blocks, grad_blocks, prefixes), reverse=True)

    def whole(array):
        return array.reshape(blocks * TOK_DEV, model_width).astype(jnp.bfloat16)
    return (normed_out, whole(grad_q), whole(grad_k), whole(grad_v))
```

```python
import functools
import jax
import jax.numpy as jnp
from jax import lax
from jax.experimental import pallas as pl
from jax.experimental.pallas import tpu as pltpu
from jax.sharding import PartitionSpec as P

DH = 128
EPSILON = 1e-06
F32 = jnp.float32
BF16 = jnp.bfloat16
CHUNKS = 2
STATS = 8


def dot_nn(a, b):
    return lax.dot_general(a, b, (((1,), (0,)), ((), ())), preferred_element_type=F32)


def dot_nt(a, b):
    return lax.dot_general(a, b, (((1,), (1,)), ((), ())), preferred_element_type=F32)


def dot_tn(a, b):
    return lax.dot_general(a, b, (((0,), (0,)), ((), ())), preferred_element_type=F32)


def columns(j):
    return slice(j * DH, (j + 1) * DH)


def outer_kernel(m_ref, a_ref, b_ref, out_ref):
    for j in range(a_ref.shape[1] // DH):
        out_ref[0, columns(j), :] = dot_tn(a_ref[:, columns(j)], b_ref[:, columns(j)])


def causal_product(rows, cols, weights, first_row, first_col, upper):
    scores = dot_nt(rows, cols)
    row_ids = first_row + lax.broadcasted_iota(jnp.int32, scores.shape, 0)
    col_ids = first_col + lax.broadcasted_iota(jnp.int32, scores.shape, 1)
    keep = col_ids >= row_ids if upper else row_ids >= col_ids
    return dot_nn(jnp.where(keep, scores, 0.0).astype(BF16), weights)


def lower(rows_ref, cols_ref, weights_ref, j, tile, r):
    here, before = slice(r * tile, (r + 1) * tile), slice(0, (r + 1) * tile)
    c = columns(j)
    return causal_product(
        rows_ref[here, c], cols_ref[before, c], weights_ref[before, c], r * tile, 0, False
    )


def upper(rows_ref, cols_ref, weights_ref, j, tile, r):
    here, after = slice(r * tile, (r + 1) * tile), slice(r * tile, None)
    c = columns(j)
    return causal_product(
        rows_ref[here, c], cols_ref[after, c], weights_ref[after, c], r * tile, r * tile, True
    )


def tile_of(tokens):
    return min(256, tokens)


def intra_kernel(m_ref, q_ref, k_ref, v_ref, out_ref):
    tile = tile_of(q_ref.shape[0])
    for j in range(q_ref.shape[1] // DH):
        for r in range(q_ref.shape[0] // tile):
            out_ref[r * tile : (r + 1) * tile, columns(j)] = lower(q_ref, k_ref, v_ref, j, tile, r)


def state_at(near_ref, far_ref, j):
    near, far = near_ref[0, columns(j), :], far_ref[0, columns(j), :]
    return jnp.where(pl.program_id(0) < 2, near, far).astype(BF16)


def attend_kernel(m_ref, q_ref, intra_ref, near_ref, far_ref, cot_ref, gain_ref, att_ref, stats_ref, acc_ref):
    p = pl.program_id(0)

    @pl.when(p == 0)
    def _():
        acc_ref[...] = jnp.zeros_like(acc_ref)

    for j in range(q_ref.shape[1] // DH):
        c = columns(j)
        att = intra_ref[:, c] + dot_nn(q_ref[:, c], state_at(near_ref, far_ref, j))
        att_ref[:, c] = att
        acc_ref[0] += att * att
        acc_ref[1] += cot_ref[:, c].astype(F32) * gain_ref[:, c] * att

    @pl.when(p == pl.num_programs(0) - 1)
    def _():
        stats_ref[...] = jnp.zeros_like(stats_ref)
        stats_ref[0:1, :] = jnp.sum(acc_ref[0].T, axis=0, keepdims=True)
        stats_ref[1:2, :] = jnp.sum(acc_ref[1].T, axis=0, keepdims=True)


def row_factors(stats_ref, model_width):
    stats = stats_ref[...].T
    inverse = 1.0 / jnp.sqrt(stats[:, 0:1] / model_width + EPSILON)
    slope = stats[:, 1:2] * inverse / model_width
    return inverse, slope


def grad_attn_kernel(model_width, m_ref, att_ref, cot_ref, gain_ref, q_ref, stats_ref, g_ref, out_ref):
    inverse, slope = row_factors(stats_ref, model_width)
    for j in range(q_ref.shape[1] // DH):
        c = columns(j)
        scaled = cot_ref[:, c].astype(F32) * gain_ref[:, c]
        grad = (inverse * (scaled - att_ref[:, c] * inverse * slope)).astype(BF16)
        g_ref[:, c] = grad
        out_ref[0, c, :] = dot_tn(q_ref[:, c], grad)


def grads_kernel(
    model_width, m_ref, q_ref, k_ref, v_ref, g_ref, near_ref, far_ref, att_ref, gain_ref, stats_ref, *rest
):
    out_ref, gq_ref, gk_ref, gv_ref = rest[-4:]
    inverse, _ = row_factors(stats_ref, model_width)
    tile = tile_of(q_ref.shape[0])
    for j in range(q_ref.shape[1] // DH):
        c = columns(j)
        out_ref[:, c] = (att_ref[:, c] * inverse * gain_ref[:, c]).astype(BF16)
        state = state_at(near_ref, far_ref, j)
        for r in range(q_ref.shape[0] // tile):
            here = slice(r * tile, (r + 1) * tile)
            grad_q = lower(g_ref, v_ref, k_ref, j, tile, r) + dot_nt(g_ref[here, c], state)
            gq_ref[here, c] = grad_q.astype(BF16)
            gk_ref[here, c] = upper(v_ref, g_ref, q_ref, j, tile, r)
            gv_ref[here, c] = upper(k_ref, q_ref, g_ref, j, tile, r)


def finish_kernel(m_ref, gki_ref, gvi_ref, k_ref, v_ref, near_ref, far_ref, *rest):
    gk_ref, gv_ref = rest[-2:]
    for j in range(k_ref.shape[1] // DH):
        c = columns(j)
        state = state_at(near_ref, far_ref, j)
        gk_ref[:, c] = (gki_ref[:, c] + dot_nt(v_ref[:, c], state)).astype(BF16)
        gv_ref[:, c] = (gvi_ref[:, c] + dot_nn(k_ref[:, c], state)).astype(BF16)


def exchange(array, mask):
    n = lax.axis_size("seq")
    return lax.ppermute(array, "seq", [(i, i ^ mask) for i in range(n)])


def outer_scan(total, reverse):
    outer = lax.axis_size("seq") // 4

    def at(z):
        return outer - 1 - z if reverse else z

    before = None
    for z in range(outer - 1):
        pairs = [(at(z) * 4 + i, at(z + 1) * 4 + i) for i in range(4)]
        got = lax.ppermute(total if before is None else total + before, "seq", pairs)
        before = got if before is None else before + got
    return before


def scan_states(state, reverse):
    me = lax.axis_index("seq")
    first_core = me & 1 == int(reverse)
    first_chip = (me >> 1) & 1 == int(reverse)
    from_core = exchange(state[2:4], 1)
    chip = state[0:2] + from_core
    from_chip = exchange(chip[1:2], 2)
    before = outer_scan(chip[0:1] + from_chip, reverse)
    mine = jnp.where(first_chip, before, before + from_chip)
    theirs = jnp.where(first_chip, before + chip[0:1], before)
    both = jnp.concatenate([mine, exchange(theirs, 2)])
    near = jnp.where(first_core, both, both + from_core)
    far = exchange(jnp.where(first_core, both + state[0:2], both), 1)
    return near, far


def body(queries, keys, values, gain, cotangent):
    tokens, width = queries.shape
    head_count = width // DH
    model_width = width * lax.axis_size("head")
    chunks = CHUNKS if head_count % (4 * CHUNKS) == 0 else 1
    wide = width // (4 * chunks)
    heads_at = wide // DH
    me = lax.axis_index("seq")
    mask = ((me & 1) * 2 + ((me >> 1) & 1)).astype(jnp.int32).reshape(1)
    gain_row = gain.reshape(1, width)

    state_shape = jax.ShapeDtypeStruct((4, wide, DH), F32)
    full16 = jax.ShapeDtypeStruct((tokens, width), BF16)
    part32 = jax.ShapeDtypeStruct((tokens, width // chunks), F32)
    part16 = jax.ShapeDtypeStruct((tokens, width // chunks), BF16)
    stats_shape = jax.ShapeDtypeStruct((STATS, tokens), F32)

    def call(kernel, c, args, specs, outs, out_specs, macs, name, scratch=(), carried=()):
        def cols(p, m):
            return (0, c * 4 + (p ^ m[0]))

        def part(p, m):
            return (0, p ^ m[0])

        kinds = {
            "x": pl.BlockSpec((tokens, wide), cols),
            "gain": pl.BlockSpec((1, wide), cols),
            "part": pl.BlockSpec((tokens, wide), part),
            "state": pl.BlockSpec((1, wide, DH), lambda p, m: (p, 0, 0)),
            "near": pl.BlockSpec((1, wide, DH), lambda p, m: (jnp.minimum(p, 1), 0, 0)),
            "far": pl.BlockSpec((1, wide, DH), lambda p, m: (jnp.maximum(p, 2) - 2, 0, 0)),
            "stats": pl.BlockSpec((STATS, tokens), lambda p, m: (0, 0)),
            "any": pl.BlockSpec(memory_space=pl.ANY),
        }
        carried = [x for x in carried if x is not None]
        in_specs = [kinds[s] for s in specs] + [kinds["any"]] * len(carried)
        first_alias = 1 + len(args)
        size = sum(x.size * x.dtype.itemsize for x in (*args, *outs)) // chunks
        return pl.pallas_call(
            kernel,
            grid_spec=pltpu.PrefetchScalarGridSpec(
                num_scalar_prefetch=1,
                grid=(4,),
                in_specs=in_specs,
                out_specs=[kinds[s] for s in out_specs],
                scratch_shapes=scratch,
            ),
            out_shape=list(outs),
            input_output_aliases={first_alias + i: i for i in range(len(carried))},
            compiler_params=pltpu.CompilerParams(
                dimension_semantics=("arbitrary",), vmem_limit_bytes=24 * 2**20
            ),
            cost_estimate=pl.CostEstimate(
                flops=2 * macs * DH * heads_at * 4, bytes_accessed=size, transcendentals=0
            ),
            name=name,
        )(mask, *args, *carried)

    every = range(chunks)
    square = tokens * tokens * 3 // 4

    states = [
        call(outer_kernel, c, (keys, values), "xx", [state_shape], ["state"], tokens * DH, f"outer{c}")[0]
        for c in every
    ]
    prefix = [scan_states(s, False) for s in states]
    intra = [
        call(
            intra_kernel, c, (queries, keys, values), "xxx", [part32], ["part"], 2 * square, f"intra{c}"
        )[0]
        for c in every
    ]
    attend, stats = zip(
        *[
            call(
                attend_kernel,
                c,
                (queries, intra[c], *prefix[c], cotangent, gain_row),
                ["x", "part", "near", "far", "x", "gain"],
                [part32, stats_shape],
                ["part", "stats"],
                tokens * DH,
                f"attend{c}",
                scratch=[pltpu.VMEM((2, tokens, DH), F32)],
            )
            for c in every
        ]
    )
    stats = functools.reduce(jnp.add, stats)
    if lax.axis_size("head") == 2:
        stats = stats + lax.ppermute(stats, "head", [(0, 1), (1, 0)])
    else:
        stats = lax.psum(stats, "head")
    grads, states = zip(
        *[
            call(
                functools.partial(grad_attn_kernel, model_width),
                c,
                (attend[c], cotangent, gain_row, queries, stats),
                ["part", "x", "gain", "x", "stats"],
                [part16, state_shape],
                ["part", "state"],
                tokens * DH,
                f"grad_attn{c}",
            )
            for c in every
        ]
    )
    suffix = [scan_states(s, True) for s in states]
    normed = grad_q = None
    inner = []
    for c in every:
        normed, grad_q, gk, gv = call(
            functools.partial(grads_kernel, model_width),
            c,
            (queries, keys, values, grads[c], *prefix[c], attend[c], gain_row, stats),
            ["x", "x", "x", "part", "near", "far", "part", "gain", "stats"],
            [full16, full16, part32, part32],
            ["x", "x", "part", "part"],
            6 * square,
            f"grads{c}",
            carried=(normed, grad_q),
        )
        inner.append((gk, gv))
    grad_k = grad_v = None
    for c in every:
        grad_k, grad_v = call(
            finish_kernel,
            c,
            (*inner[c], keys, values, *suffix[c]),
            ["part", "part", "x", "x", "near", "far"],
            [full16, full16],
            ["x", "x"],
            2 * tokens * DH,
            f"finish{c}",
            carried=(grad_k, grad_v),
        )
    return normed, grad_q, grad_k, grad_v


def solution(mesh):
    spec = P("seq", "head")
    in_specs = (spec, spec, spec, P("head"), spec)
    return jax.shard_map(body, mesh=mesh, in_specs=in_specs, out_specs=(spec,) * 4, check_vma=False)
```
